32 devices in a mesh: lon: 8 (over y, x, core), lat: 4 (over z).
Axes of the slice: x: 2, y: 2, z: 4, core: 2. Of those that a mesh axis runs over, the one named last changes fastest.
Arguments:
- surface_forcing: float32 [96, 1024], P('lat', 'lon'), may hold values from -33 to 33
- sea_mask: int32 [96, 1024], P('lat', 'lon'), may hold values 0 or 1
- level_count: int32 [96, 1024], P('lat', 'lon'), may hold values from 1 to 40
- state: float32 [4, 40, 96, 1024], P(None, None, 'lat', 'lon'), may hold values from -6 to 6
Outputs:
- surface_height: float32 [96, 1024], P('lat', 'lon')
- residual: float32 [96, 1024], P('lat', 'lon')
- tendency: float32 [4, 40, 96, 1024], P(None, None, 'lat', 'lon')
The draws below stay inside these ranges and needn't reach their ends.
All inputs are finite; a program needn't handle non-finite values. No bound on the sum of `sea_mask` on one device may be relied on, other than what follows from the above.
Results may differ from the reference program's by a relative error of at most 0.0003.
Values sent between devices are 32-bit elements; how exact they have to be, the bound alone decides.
No kernel may reach another device: no remote copies, remote signals or barrier semaphores. Data moves between devices by JAX's collectives and lax.ppermute only.
A program may use at most 64 MiB of HBM per device.

```python
import jax
import jax.numpy as jnp
from jax import lax

LEV = 40
ITERS = 4
NX = 1024
NY = 96


def draw_surface_forcing(key, part):
    row_frac = jnp.arange(NY, dtype=jnp.float32) / NY
    column_frac = jnp.arange(NX, dtype=jnp.float32) / NX
    growth = jnp.exp(jnp.log(3.0) * (row_frac[:, None] + column_frac[None, :]))
    key_rough = jax.random.fold_in(jax.random.fold_in(key, 11), 0)
    values = jax.random.truncated_normal(key_rough, -3.0, 3.0, (NY, NX), jnp.float32) * growth
    return values


def plant(values, own_key, least, top_value):
    spot = [jax.random.randint(jax.random.fold_in(own_key, axis), (), 0, length) for axis, length in enumerate(values.shape)]
    main_axis = values.shape.index(max(values.shape))
    neighbour = spot[:main_axis] + [(spot[main_axis] + 1) % values.shape[main_axis]] + spot[main_axis + 1:]
    return values.at[tuple(spot)].set(least).at[tuple(neighbour)].set(top_value)


def shard_levels(key, shape, pieces, low, largest):
    def one(axis_at, parts):
        draws = jax.random.uniform(jax.random.fold_in(jax.random.fold_in(key, 6), axis_at), (parts,), jnp.float32, low / len(pieces), largest / len(pieces))
        return jnp.repeat(jnp.exp(draws), shape[axis_at] // parts).reshape((-1,) + (1,) * (len(shape) - axis_at - 1))

    gain = one(*pieces[0])
    for cut in pieces[1:]:
        gain = gain * one(*cut)
    return gain


def centred(key, dims, scale, most, cuts=(), kind=jnp.bfloat16):
    entries = scale * jax.random.normal(key, dims, jnp.float32)
    if cuts:
        entries = entries * shard_levels(key, dims, cuts, -0.22, 0.18)
    return jnp.clip(entries, -most, most).astype(kind)


def setup_inputs(seed: int = 0) -> dict:
    arg_keys = jax.random.split(jax.random.key(seed), 5)
    return {
        "surface_forcing": draw_surface_forcing(jax.random.fold_in(arg_keys[4], 71), 0),
        "sea_mask": plant((jax.random.randint(arg_keys[1], (NY, NX), 0, 4) < 3).astype(jnp.int32), jax.random.fold_in(arg_keys[1], 1), 0, 1),
        "level_count": plant(jax.random.randint(arg_keys[2], (NY, NX), 1, LEV + 1), jax.random.fold_in(arg_keys[2], 1), 1, LEV).astype(jnp.int32),
        "state": centred(arg_keys[3], (4, LEV, NY, NX), 1.0, 6.0, ((2, 4), (3, 8)), jnp.float32),
    }


damping = 0.05
face_scale = 1.0
viscosity = 0.02


def wrap_pad(field, width):
    field = jnp.concatenate([field[..., -width:], field, field[..., :width]], axis=-1)
    spec = [(0, 0)] * (field.ndim - 2) + [(width, width), (0, 0)]
    return jnp.pad(field, spec)


def trim_rims(field, margin):
    return field[..., margin:field.shape[-2] - margin, margin:field.shape[-1] - margin]


def face_coeffs(depth, width_out, width_in):
    offset = width_in - width_out
    height = depth.shape[0] - 2 * offset
    breadth = depth.shape[1] - 2 * offset
    center = depth[offset:offset + height, offset:offset + breadth]
    east_face = face_scale * jnp.minimum(center, depth[offset:offset + height, offset + 1:offset + 1 + breadth])
    west_face = face_scale * jnp.minimum(center, depth[offset:offset + height, offset - 1:offset - 1 + breadth])
    north_face = face_scale * jnp.minimum(center, depth[offset + 1:offset + 1 + height, offset:offset + breadth])
    south_face = face_scale * jnp.minimum(center, depth[offset - 1:offset - 1 + height, offset:offset + breadth])
    diagonal = damping + east_face + west_face + north_face + south_face
    return diagonal, east_face, west_face, north_face, south_face


def operator_apply(padded, coeffs):
    diagonal, east_face, west_face, north_face, south_face = coeffs
    return (diagonal * padded[1:-1, 1:-1] - east_face * padded[1:-1, 2:] - west_face * padded[1:-1, :-2]
            - north_face * padded[2:, 1:-1] - south_face * padded[:-2, 1:-1])


def laplace(field, active):
    center = field[..., 1:-1, 1:-1]
    active_center = active[..., 1:-1, 1:-1]
    east_part = active_center * active[..., 1:-1, 2:] * (field[..., 1:-1, 2:] - center)
    west_part = active_center * active[..., 1:-1, :-2] * (center - field[..., 1:-1, :-2])
    north_part = active_center * active[..., 2:, 1:-1] * (field[..., 2:, 1:-1] - center)
    south_part = active_center * active[..., :-2, 1:-1] * (center - field[..., :-2, 1:-1])
    return east_part - west_part + north_part - south_part


def advect(field, active):
    east_flow = field[2]
    north_flow = field[3]
    center = field[..., 1:-1, 1:-1]
    active_center = active[..., 1:-1, 1:-1]
    flow_center = east_flow[..., 1:-1, 1:-1]
    lift_center = north_flow[..., 1:-1, 1:-1]
    east_speed = 0.25 * active_center * active[..., 1:-1, 2:] * (flow_center + east_flow[..., 1:-1, 2:])
    west_speed = 0.25 * active_center * active[..., 1:-1, :-2] * (flow_center + east_flow[..., 1:-1, :-2])
    north_speed = 0.25 * active_center * active[..., 2:, 1:-1] * (lift_center + north_flow[..., 2:, 1:-1])
    south_speed = 0.25 * active_center * active[..., :-2, 1:-1] * (lift_center + north_flow[..., :-2, 1:-1])
    return (east_speed * (center + field[..., 1:-1, 2:]) - west_speed * (center + field[..., 1:-1, :-2])
            + north_speed * (center + field[..., 2:, 1:-1]) - south_speed * (center + field[..., :-2, 1:-1]))


def tendency_of(state_wide, active_wide):
    inner_active = trim_rims(active_wide, 1)
    smoothed = laplace(laplace(state_wide, active_wide), inner_active)
    flux = advect(trim_rims(state_wide, 1), inner_active)
    return trim_rims(active_wide, 2) * (-flux - viscosity * smoothed)


def reference(surface_forcing, sea_mask, level_count, state):
    sea = sea_mask.astype(jnp.float32)
    depth = sea * level_count.astype(jnp.float32) / LEV
    coeffs = face_coeffs(wrap_pad(depth, 1), 0, 1)
    forcing = sea * surface_forcing
    solution = jnp.zeros_like(forcing)
    residual = forcing
    search = residual / coeffs[0]
    direction = search
    product = jnp.sum(residual * search)
    for step_index in range(ITERS):
        image = operator_apply(wrap_pad(direction, 1), coeffs)
        alpha_step = product / jnp.sum(direction * image)
        solution = solution + alpha_step * direction
        residual = residual - alpha_step * image
        if step_index + 1 < ITERS:
            search = residual / coeffs[0]
            product_next = jnp.sum(residual * search)
            direction = search + (product_next / product) * direction
            product = product_next

    def level_tendency(level):
        active = (level < level_count).astype(jnp.float32) * sea
        layer = lax.dynamic_index_in_dim(state, level, 1, keepdims=False)
        return tendency_of(wrap_pad(layer, 2), wrap_pad(active, 2))

    stacked = lax.map(level_tendency, jnp.arange(LEV, dtype=jnp.int32))
    return solution, residual, jnp.moveaxis(stacked, 0, 1)
```

```python
import functools

import jax
import jax.numpy as jnp
from jax import lax
from jax.experimental import pallas as pl
from jax.experimental.pallas import tpu as pltpu
from jax.sharding import PartitionSpec as P

ITERS = 4
damping = 0.05
viscosity = 0.02
LEVEL_BLOCK = 8
HALF = 64


def lane_iota(shape):
    return lax.broadcasted_iota(jnp.int32, shape, 1)


def pick_block(levels):
    return LEVEL_BLOCK if levels % LEVEL_BLOCK == 0 else 1


def pack_kernel(force_ref, sea_ref, count_ref, state_ref, north_ref, south_ref, pair_ref, cols_ref, *, levels):
    step = pl.program_id(0)
    fields, block, height, width = state_ref.shape

    @pl.when(step == 0)
    def _():
        sea = sea_ref[...].astype(jnp.float32)
        wet = sea * count_ref[...].astype(jnp.float32)
        forcing = sea * force_ref[...]
        half = height // 2
        for n in range(half):
            rows = slice(2 * n, 2 * n + 2)
            for ref, start in ((north_ref, fields * levels), (south_ref, fields * levels), (pair_ref, 0)):
                ref[start + n] = forcing[rows]
                ref[start + half + n] = wet[rows]
        cols_ref[...] = jnp.zeros(cols_ref.shape, jnp.float32)

    lane = lane_iota((height, width))
    edges = (0, 1, width - 2, width - 1)
    held = [[cols_ref[c, p] for p in range(fields // 2)] for c in range(4)]
    for kk in range(block):
        level = step * block + kk
        for f in range(fields):
            x = state_ref[f, kk]
            north_ref[f * levels + level] = x[height - 2 :]
            south_ref[f * levels + level] = x[:2]
            spot = (f % 2) * HALF + level
            mine = lane == spot
            for c, edge in enumerate(edges):
                moved = pltpu.roll(x, lax.rem(spot + (width - edge), width), 1)
                held[c][f // 2] = jnp.where(mine, moved, held[c][f // 2])
    for c in range(4):
        for p in range(fields // 2):
            cols_ref[c, p] = held[c][p]


def middle_kernel(*refs, levels, fields, lats):
    place_ref, cols_ref, own_ref = refs[:3]
    others = refs[3 : 3 + lats - 1]
    halo_ref, wide_ref, west_ref, east_ref, grid_ref, tall = refs[3 + lats - 1 :]
    height, width = cols_ref.shape[2:]
    half = height // 2
    base = fields * levels
    north, south = others[0], others[lats - 2]
    for b in range(lats):
        source = own_ref if b == 0 else others[b - 1]
        start = base if b in (1, lats - 1) else 0
        for n in range(height):
            grid_ref[b * 2 * height + 2 * n : b * 2 * height + 2 * n + 2] = source[start + n]
    lat = place_ref[0]
    wide_ref[:height] = grid_ref[height : 2 * height]
    wide_ref[height:] = jnp.zeros((8, width), jnp.float32)

    @pl.when(lat < lats - 1)
    def _():
        wide_ref[height : height + 2] = north[base + half]

    @pl.when(lat > 0)
    def _():
        wide_ref[height + 6 : height + 8] = south[base + height - 1]

    lane8 = lane_iota((8, width))
    near = [[jnp.zeros((8, width), jnp.float32) for _ in range(fields // 2)] for _ in range(2)]
    empty = jnp.zeros((4, width), jnp.float32)
    for f in range(fields):
        for k in range(levels):
            n = f * levels + k
            halo_ref[f, k, 0:2] = north[n]
            halo_ref[f, k, 2:6] = empty
            halo_ref[f, k, 6:8] = south[n]
    for f in range(fields):
        for k in range(levels):
            x = halo_ref[f, k]
            spot = (f % 2) * HALF + k
            for c, edge in enumerate((0, width - 1)):
                near[c][f // 2] = jnp.where(lane8 == spot, pltpu.roll(x, (spot - edge) % width, 1), near[c][f // 2])
    tall_rows = height + 8
    wide = wide_ref[...]
    lane_tall = lane_iota((tall_rows, width))
    for out_ref, c_near, c_far, edge_near, edge_far, slot in (
        (west_ref, 0, 1, 0, 1, 0),
        (east_ref, 3, 2, width - 1, width - 2, 1),
    ):
        for p in range(fields // 2):
            tall[:height] = cols_ref[c_near, p]
            tall[height:] = near[slot][p]
            value = tall[...]
            tall[:height] = cols_ref[c_far, p]
            tall[height:] = jnp.zeros((8, width), jnp.float32)
            value_far = tall[...]
            if p == 0:
                value = jnp.where(lane_tall == levels, pltpu.roll(wide, (levels - edge_near) % width, 1), value)
                value_far = jnp.where(lane_tall == levels, pltpu.roll(wide, (levels - edge_far) % width, 1), value_far)
            out_ref[p * tall_rows : (p + 1) * tall_rows] = value
            q = fields // 2 + p
            out_ref[q * tall_rows : (q + 1) * tall_rows] = value_far
        out_ref[2 * (fields // 2) * tall_rows :] = grid_ref[...]


def tendency_kernel(state_ref, halo_ref, wide_ref, own_w_ref, own_e_ref, got_w_ref, got_e_ref, out_ref, faces, edge_lap, *, levels):
    step = pl.program_id(0)
    fields, block, height, width = state_ref.shape
    rows = height + 8
    pairs = fields // 2
    lane = lane_iota((rows, width))
    last, first = lane == width - 1, lane == 0

    def part(ref, far, p):
        q = (pairs if far else 0) + p
        return ref[q * rows : (q + 1) * rows]

    def up(x):
        return pltpu.roll(x, rows - 1, 0)

    def down(x):
        return pltpu.roll(x, 1, 0)

    @pl.when(step == 0)
    def _():
        wide = wide_ref[...]
        east = jnp.where(last, pltpu.roll(part(got_e_ref, False, 0), width - 1 - levels, 1), pltpu.roll(wide, width - 1, 1))
        west = jnp.where(first, pltpu.roll(part(got_w_ref, False, 0), width - levels, 1), pltpu.roll(wide, 1, 1))
        for n, other in enumerate((east, west, up(wide), down(wide))):
            faces[n] = jnp.minimum(wide, other)
        depth_at = lax.rem(lane, HALF).astype(jnp.float32)
        for side, (got, own, sign) in enumerate(((got_w_ref, own_w_ref, 1.0), (got_e_ref, own_e_ref, -1.0))):
            wet_near, wet_far, wet_own = (
                jnp.broadcast_to(part(ref, far, 0)[:, levels : levels + 1], (rows, width))
                for ref, far in ((got, False), (got, True), (own, False))
            )
            masks = [depth_at < jnp.minimum(wet_near, other) for other in (wet_own, wet_far, up(wet_near), down(wet_near))]
            for p in range(pairs):
                here, beyond, inner = part(got, False, p), part(got, True, p), part(own, False, p)
                total = jnp.zeros((rows, width), jnp.float32)
                for mask, other in zip(masks, (inner, beyond, up(here), down(here))):
                    total = total + jnp.where(mask, other - here, 0.0)
                edge_lap[side, p] = total

    wide = wide_ref[...]
    low = slice(0, height)
    for kk in range(block):
        level = step * block + kk
        depth = level.astype(jnp.float32)
        on_e, on_w, on_n, on_s = (depth < faces[n] for n in range(4))
        here_on = depth < wide[low]
        around = []
        for f in range(fields):
            x = jnp.concatenate([state_ref[f, kk], halo_ref[f, kk]], axis=0)
            spot = (f % 2) * HALF + level
            p = f // 2
            east = jnp.where(last, pltpu.roll(part(got_e_ref, False, p), width - 1 - spot, 1), pltpu.roll(x, width - 1, 1))
            west = jnp.where(first, pltpu.roll(part(got_w_ref, False, p), lax.rem(width - spot, width), 1), pltpu.roll(x, 1, 1))
            around.append((x, east, west, up(x), down(x)))
        u, v = around[2], around[3]
        mask_low = [m[low] for m in (on_e, on_w, on_n, on_s)]
        speed = [
            jnp.where(mask_low[0], 0.25 * (u[0][low] + u[1][low]), 0.0),
            jnp.where(mask_low[1], 0.25 * (u[0][low] + u[2][low]), 0.0),
            jnp.where(mask_low[2], 0.25 * (v[0][low] + v[3][low]), 0.0),
            jnp.where(mask_low[3], 0.25 * (v[0][low] + v[4][low]), 0.0),
        ]
        for f in range(fields):
            x, east, west, north, south = around[f]
            spot = (f % 2) * HALF + level
            p = f // 2
            lap = (
                jnp.where(on_e, east - x, 0.0)
                - jnp.where(on_w, x - west, 0.0)
                + jnp.where(on_n, north - x, 0.0)
                - jnp.where(on_s, x - south, 0.0)
            )
            inner = lap[low]
            lap_e = jnp.where(last[low], pltpu.roll(edge_lap[1, p][low], width - 1 - spot, 1), pltpu.roll(inner, width - 1, 1))
            lap_w = jnp.where(first[low], pltpu.roll(edge_lap[0, p][low], lax.rem(width - spot, width), 1), pltpu.roll(inner, 1, 1))
            lap_n, lap_s = up(lap)[low], down(lap)[low]
            second = (
                jnp.where(mask_low[0], lap_e - inner, 0.0)
                - jnp.where(mask_low[1], inner - lap_w, 0.0)
                + jnp.where(mask_low[2], lap_n - inner, 0.0)
                - jnp.where(mask_low[3], inner - lap_s, 0.0)
            )
            q = x[low]
            flux = (
                speed[0] * (q + east[low])
                - speed[1] * (q + west[low])
                + speed[2] * (q + north[low])
                - speed[3] * (q + south[low])
            )
            out_ref[f, kk] = jnp.where(here_on, -flux - viscosity * second, 0.0)


def solve_kernel(*refs, levels, lats, lons, height, width):
    place_ref = refs[0]
    sources = refs[1 : 1 + lons]
    height_ref, residual_ref = refs[1 + lons : 3 + lons]
    depth_ref, east_ref, west_ref, north_ref, south_ref, diag_ref, r_ref, p_ref = refs[3 + lons :]
    tall, broad = lats * height, lons * width
    for d, source in enumerate(sources):
        start = source.shape[0] - lats * 2 * height
        for b in range(lats):
            at = start + b * 2 * height
            block = (slice(b * height, (b + 1) * height), slice(d * width, (d + 1) * width))
            r_ref[block] = source[at : at + height]
            depth_ref[block] = source[at + height : at + 2 * height] / levels

    def to_east(x):
        return pltpu.roll(x, broad - 1, 1)

    def to_west(x):
        return pltpu.roll(x, 1, 1)

    def to_north(x):
        return pltpu.roll(x, tall - 1, 0)

    def to_south(x):
        return pltpu.roll(x, 1, 0)

    depth = depth_ref[...]
    row = lax.rem(lax.broadcasted_iota(jnp.int32, (tall, broad), 0) + place_ref[0] * height, tall)
    east_ref[...] = jnp.minimum(depth, to_east(depth))
    west_ref[...] = jnp.minimum(depth, to_west(depth))
    north_ref[...] = jnp.where(row == tall - 1, 0.0, jnp.minimum(depth, to_north(depth)))
    south_ref[...] = jnp.where(row == 0, 0.0, jnp.minimum(depth, to_south(depth)))
    diag_ref[...] = damping + east_ref[...] + west_ref[...] + north_ref[...] + south_ref[...]
    depth_ref[...] = 1.0 / diag_ref[...]
    inverse_ref = depth_ref
    search = r_ref[...] * inverse_ref[...]
    p_ref[...] = search

    def total(x):
        return jnp.sum(jnp.sum(x, axis=0, keepdims=True), axis=1, keepdims=True)

    product = total(r_ref[...] * search)

    def advance(product, answer):
        p = p_ref[...]
        image = (
            diag_ref[...] * p
            - east_ref[...] * to_east(p)
            - west_ref[...] * to_west(p)
            - north_ref[...] * to_north(p)
            - south_ref[...] * to_south(p)
        )
        alpha = product / total(p * image)
        answer = answer + alpha * p_ref[:height, :width]
        r_ref[...] = r_ref[...] - alpha * image
        return answer

    def step(_, carry):
        product, answer = carry
        answer = advance(product, answer)
        search = r_ref[...] * inverse_ref[...]
        new = total(r_ref[...] * search)
        p_ref[...] = search + (new / product) * p_ref[...]
        return new, answer

    product, answer = lax.fori_loop(0, ITERS - 1, step, (product, jnp.zeros((height, width), jnp.float32)))
    height_ref[...] = advance(product, answer)
    residual_ref[...] = r_ref[:height, :width]


def shifted(x, axis, distance):
    count = lax.axis_size(axis)
    return lax.ppermute(x, axis, [((i + distance) % count, i) for i in range(count)])


def per_device(surface_forcing, sea_mask, level_count, state):
    fields, levels, height, width = state.shape
    lats, lons = lax.axis_size("lat"), lax.axis_size("lon")
    block = pick_block(levels)
    f32 = jnp.float32
    pairs = fields // 2
    rows = height + 8
    whole = lambda shape: pl.BlockSpec(shape, lambda i: (0,) * len(shape))
    message = (fields * levels + height, 2, width)
    north_msg, south_msg, pair, cols = pl.pallas_call(
        functools.partial(pack_kernel, levels=levels),
        grid=(levels // block,),
        in_specs=[whole((height, width))] * 3 + [pl.BlockSpec((fields, block, height, width), lambda i: (0, i, 0, 0))],
        out_specs=[whole(message), whole(message), whole((height, 2, width)), whole((4, pairs, height, width))],
        out_shape=[
            jax.ShapeDtypeStruct(message, f32),
            jax.ShapeDtypeStruct(message, f32),
            jax.ShapeDtypeStruct((height, 2, width), f32),
            jax.ShapeDtypeStruct((4, pairs, height, width), f32),
        ],
        name="pack",
    )(surface_forcing, sea_mask, level_count, state)

    place = lax.axis_index("lat").astype(jnp.int32)[None]
    from_lat = [
        shifted(south_msg if b == 1 else north_msg if b == lats - 1 else pair, "lat", b) for b in range(1, lats)
    ]
    smem = pl.BlockSpec(memory_space=pltpu.SMEM)
    vmem = pl.BlockSpec(memory_space=pltpu.VMEM)
    strip = 2 * pairs * rows
    cells = lats * 2 * height
    halo, wide, west_msg, east_msg, grid = pl.pallas_call(
        functools.partial(middle_kernel, levels=levels, fields=fields, lats=lats),
        in_specs=[smem] + [vmem] * (2 + lats - 1),
        out_specs=[vmem] * 5,
        out_shape=[
            jax.ShapeDtypeStruct((fields, levels, 8, width), f32),
            jax.ShapeDtypeStruct((rows, width), f32),
            jax.ShapeDtypeStruct((strip + cells, width), f32),
            jax.ShapeDtypeStruct((strip + cells, width), f32),
            jax.ShapeDtypeStruct((cells, width), f32),
        ],
        scratch_shapes=[pltpu.VMEM((rows, width), f32)],
        name="middle",
    )(place, cols, pair, *from_lat)

    order = [1, lons - 1] + list(range(2, lons - 1))
    got = {d: shifted(west_msg if d == 1 else east_msg if d == lons - 1 else grid, "lon", d) for d in order}
    tendency = pl.pallas_call(
        functools.partial(tendency_kernel, levels=levels),
        grid=(levels // block,),
        in_specs=[
            pl.BlockSpec((fields, block, height, width), lambda i: (0, i, 0, 0)),
            pl.BlockSpec((fields, block, 8, width), lambda i: (0, i, 0, 0)),
            whole((rows, width)),
        ]
        + [whole((strip, width))] * 4,
        out_specs=pl.BlockSpec((fields, block, height, width), lambda i: (0, i, 0, 0)),
        out_shape=jax.ShapeDtypeStruct(state.shape, f32),
        scratch_shapes=[pltpu.VMEM((4, rows, width), f32), pltpu.VMEM((2, pairs, rows, width), f32)],
        cost_estimate=pl.CostEstimate(flops=100 * state.size, bytes_accessed=9 * state.size, transcendentals=0),
        name="tendency",
    )(state, halo, wide, west_msg, east_msg, got[lons - 1], got[1])

    field = pltpu.VMEM((lats * height, lons * width), f32)
    surface, residual = pl.pallas_call(
        functools.partial(solve_kernel, levels=levels, lats=lats, lons=lons, height=height, width=width),
        in_specs=[smem] + [vmem] * lons,
        out_specs=[vmem] * 2,
        out_shape=[jax.ShapeDtypeStruct((height, width), f32)] * 2,
        scratch_shapes=[field] * 8,
        name="solve",
    )(place, grid, *[got[d] for d in range(1, lons)])
    return surface, residual, tendency


def solution(mesh):
    return jax.shard_map(
        per_device,
        mesh=mesh,
        in_specs=(P("lat", "lon"), P("lat", "lon"), P("lat", "lon"), P(None, None, "lat", "lon")),
        out_specs=(P("lat", "lon"), P("lat", "lon"), P(None, None, "lat", "lon")),
        check_vma=False,
    )
```

```python
import functools

import jax
import jax.numpy as jnp
from jax import lax
from jax.experimental import pallas as pl
from jax.experimental.pallas import tpu as pltpu
from jax.sharding import PartitionSpec as P

ITERS = 4
damping = 0.05
viscosity = 0.02
LEVEL_BLOCK = 8
HALF = 64


def lane_iota(shape):
    return lax.broadcasted_iota(jnp.int32, shape, 1)


def pick_block(levels):
    return LEVEL_BLOCK if levels % LEVEL_BLOCK == 0 else 1


def pack_kernel(
    force_ref, sea_ref, count_ref, state_ref, up_ref, down_ref, north_ref, south_ref, pair_ref, cols_ref, *, levels
):
    step = pl.program_id(0)
    fields, block, height, width = state_ref.shape

    @pl.when(step == 0)
    def _():
        sea = sea_ref[...].astype(jnp.float32)
        wet = sea * count_ref[...].astype(jnp.float32)
        forcing = sea * force_ref[...]
        half = height // 2
        for n in range(half):
            rows = slice(2 * n, 2 * n + 2)
            for ref in (north_ref, south_ref, pair_ref):
                ref[n] = forcing[rows]
                ref[half + n] = wet[rows]
        cols_ref[...] = jnp.zeros(cols_ref.shape, jnp.float32)

    lane = lane_iota((height, width))
    edges = (0, 1, width - 2, width - 1)
    held = [[cols_ref[c, p] for p in range(fields // 2)] for c in range(4)]
    for kk in range(block):
        level = step * block + kk
        for f in range(fields):
            x = state_ref[f, kk]
            up_ref[f, kk] = x[height - 2 :]
            down_ref[f, kk] = x[:2]
            spot = (f % 2) * HALF + level
            mine = lane == spot
            for c, edge in enumerate(edges):
                moved = pltpu.roll(x, lax.rem(spot + (width - edge), width), 1)
                held[c][f // 2] = jnp.where(mine, moved, held[c][f // 2])
    for c in range(4):
        for p in range(fields // 2):
            cols_ref[c, p] = held[c][p]
    for slot, c in enumerate((0, 3)):
        for p in range(fields // 2):
            north_ref[height + slot, p : p + 1] = held[c][p][height - 1 :]
            south_ref[height + slot, p : p + 1] = held[c][p][:1]


def middle_kernel(*refs, levels, fields, lats):
    place_ref, cols_ref, own_ref = refs[:3]
    others = refs[3 : 3 + lats - 1]
    wide_ref, west_ref, east_ref, grid_ref, tall = refs[3 + lats - 1 :]
    height, width = cols_ref.shape[2:]
    half = height // 2
    north, south = others[0], others[lats - 2]
    for b in range(lats):
        source = own_ref if b == 0 else others[b - 1]
        for n in range(height):
            grid_ref[b * 2 * height + 2 * n : b * 2 * height + 2 * n + 2] = source[n]
    lat = place_ref[0]
    wide_ref[:height] = grid_ref[height : 2 * height]
    wide_ref[height:] = jnp.zeros((8, width), jnp.float32)

    @pl.when(lat < lats - 1)
    def _():
        wide_ref[height : height + 2] = north[half]

    @pl.when(lat > 0)
    def _():
        wide_ref[height + 6 : height + 8] = south[height - 1]

    tall_rows = height + 8
    wide = wide_ref[...]
    lane_tall = lane_iota((tall_rows, width))
    for out_ref, c_near, c_far, edge_near, edge_far, slot in (
        (west_ref, 0, 1, 0, 1, 0),
        (east_ref, 3, 2, width - 1, width - 2, 1),
    ):
        for p in range(fields // 2):
            tall[:height] = cols_ref[c_near, p]
            tall[height:] = jnp.zeros((8, width), jnp.float32)
            tall[height : height + 1] = north[height + slot, p : p + 1]
            tall[height + 7 :] = south[height + slot, p : p + 1]
            value = tall[...]
            tall[:height] = cols_ref[c_far, p]
            tall[height:] = jnp.zeros((8, width), jnp.float32)
            value_far = tall[...]
            if p == 0:
                value = jnp.where(lane_tall == levels, pltpu.roll(wide, (levels - edge_near) % width, 1), value)
                value_far = jnp.where(lane_tall == levels, pltpu.roll(wide, (levels - edge_far) % width, 1), value_far)
            out_ref[p * tall_rows : (p + 1) * tall_rows] = value
            q = fields // 2 + p
            out_ref[q * tall_rows : (q + 1) * tall_rows] = value_far
        out_ref[2 * (fields // 2) * tall_rows :] = grid_ref[...]


def tendency_kernel(
    state_ref, below_ref, above_ref, wide_ref, own_w_ref, own_e_ref, got_w_ref, got_e_ref, out_ref, faces, edge_lap, halo, *, levels
):
    step = pl.program_id(0)
    fields, block, height, width = state_ref.shape
    rows = height + 8
    pairs = fields // 2
    lane = lane_iota((rows, width))
    last, first = lane == width - 1, lane == 0

    def part(ref, far, p):
        q = (pairs if far else 0) + p
        return ref[q * rows : (q + 1) * rows]

    def up(x):
        return pltpu.roll(x, rows - 1, 0)

    def down(x):
        return pltpu.roll(x, 1, 0)

    @pl.when(step == 0)
    def _():
        halo[...] = jnp.zeros(halo.shape, jnp.float32)
        wide = wide_ref[...]
        east = jnp.where(last, pltpu.roll(part(got_e_ref, False, 0), width - 1 - levels, 1), pltpu.roll(wide, width - 1, 1))
        west = jnp.where(first, pltpu.roll(part(got_w_ref, False, 0), width - levels, 1), pltpu.roll(wide, 1, 1))
        for n, other in enumerate((east, west, up(wide), down(wide))):
            faces[n] = jnp.minimum(wide, other)
        depth_at = lax.rem(lane, HALF).astype(jnp.float32)
        for side, (got, own, sign) in enumerate(((got_w_ref, own_w_ref, 1.0), (got_e_ref, own_e_ref, -1.0))):
            wet_near, wet_far, wet_own = (
                jnp.broadcast_to(part(ref, far, 0)[:, levels : levels + 1], (rows, width))
                for ref, far in ((got, False), (got, True), (own, False))
            )
            masks = [depth_at < jnp.minimum(wet_near, other) for other in (wet_own, wet_far, up(wet_near), down(wet_near))]
            for p in range(pairs):
                here, beyond, inner = part(got, False, p), part(got, True, p), part(own, False, p)
                total = jnp.zeros((rows, width), jnp.float32)
                for mask, other in zip(masks, (inner, beyond, up(here), down(here))):
                    total = total + jnp.where(mask, other - here, 0.0)
                edge_lap[side, p] = total

    wide = wide_ref[...]
    low = slice(0, height)
    for kk in range(block):
        for f in range(fields):
            halo[f, kk, 0:2] = above_ref[f, kk]
            halo[f, kk, 6:8] = below_ref[f, kk]
    for kk in range(block):
        level = step * block + kk
        depth = level.astype(jnp.float32)
        on_e, on_w, on_n, on_s = (depth < faces[n] for n in range(4))
        here_on = depth < wide[low]
        around = []
        for f in range(fields):
            x = jnp.concatenate([state_ref[f, kk], halo[f, kk]], axis=0)
            spot = (f % 2) * HALF + level
            p = f // 2
            east = jnp.where(last, pltpu.roll(part(got_e_ref, False, p), width - 1 - spot, 1), pltpu.roll(x, width - 1, 1))
            west = jnp.where(first, pltpu.roll(part(got_w_ref, False, p), lax.rem(width - spot, width), 1), pltpu.roll(x, 1, 1))
            around.append((x, east, west, up(x), down(x)))
        u, v = around[2], around[3]
        mask_low = [m[low] for m in (on_e, on_w, on_n, on_s)]
        speed = [
            jnp.where(mask_low[0], 0.25 * (u[0][low] + u[1][low]), 0.0),
            jnp.where(mask_low[1], 0.25 * (u[0][low] + u[2][low]), 0.0),
            jnp.where(mask_low[2], 0.25 * (v[0][low] + v[3][low]), 0.0),
            jnp.where(mask_low[3], 0.25 * (v[0][low] + v[4][low]), 0.0),
        ]
        for f in range(fields):
            x, east, west, north, south = around[f]
            spot = (f % 2) * HALF + level
            p = f // 2
            lap = (
                jnp.where(on_e, east - x, 0.0)
                - jnp.where(on_w, x - west, 0.0)
                + jnp.where(on_n, north - x, 0.0)
                - jnp.where(on_s, x - south, 0.0)
            )
            inner = lap[low]
            lap_e = jnp.where(last[low], pltpu.roll(edge_lap[1, p][low], width - 1 - spot, 1), pltpu.roll(inner, width - 1, 1))
            lap_w = jnp.where(first[low], pltpu.roll(edge_lap[0, p][low], lax.rem(width - spot, width), 1), pltpu.roll(inner, 1, 1))
            lap_n, lap_s = up(lap)[low], down(lap)[low]
            second = (
                jnp.where(mask_low[0], lap_e - inner, 0.0)
                - jnp.where(mask_low[1], inner - lap_w, 0.0)
                + jnp.where(mask_low[2], lap_n - inner, 0.0)
                - jnp.where(mask_low[3], inner - lap_s, 0.0)
            )
            q = x[low]
            flux = (
                speed[0] * (q + east[low])
                - speed[1] * (q + west[low])
                + speed[2] * (q + north[low])
                - speed[3] * (q + south[low])
            )
            out_ref[f, kk] = jnp.where(here_on, -flux - viscosity * second, 0.0)


def solve_kernel(*refs, levels, lats, lons, height, width):
    place_ref = refs[0]
    sources = refs[1 : 1 + lons]
    height_ref, residual_ref = refs[1 + lons : 3 + lons]
    depth_ref, east_ref, west_ref, north_ref, south_ref, diag_ref, r_ref, p_ref = refs[3 + lons :]
    tall, broad = lats * height, lons * width
    for d, source in enumerate(sources):
        start = source.shape[0] - lats * 2 * height
        for b in range(lats):
            at = start + b * 2 * height
            block = (slice(b * height, (b + 1) * height), slice(d * width, (d + 1) * width))
            r_ref[block] = source[at : at + height]
            depth_ref[block] = source[at + height : at + 2 * height] / levels

    def to_east(x):
        return pltpu.roll(x, broad - 1, 1)

    def to_west(x):
        return pltpu.roll(x, 1, 1)

    def to_north(x):
        return pltpu.roll(x, tall - 1, 0)

    def to_south(x):
        return pltpu.roll(x, 1, 0)

    depth = depth_ref[...]
    row = lax.rem(lax.broadcasted_iota(jnp.int32, (tall, broad), 0) + place_ref[0] * height, tall)
    east_ref[...] = jnp.minimum(depth, to_east(depth))
    west_ref[...] = jnp.minimum(depth, to_west(depth))
    north_ref[...] = jnp.where(row == tall - 1, 0.0, jnp.minimum(depth, to_north(depth)))
    south_ref[...] = jnp.where(row == 0, 0.0, jnp.minimum(depth, to_south(depth)))
    diag_ref[...] = damping + east_ref[...] + west_ref[...] + north_ref[...] + south_ref[...]
    depth_ref[...] = 1.0 / diag_ref[...]
    inverse_ref = depth_ref
    search = r_ref[...] * inverse_ref[...]
    p_ref[...] = search

    def total(x):
        return jnp.sum(jnp.sum(x, axis=0, keepdims=True), axis=1, keepdims=True)

    product = total(r_ref[...] * search)

    def advance(product, answer):
        p = p_ref[...]
        image = (
            diag_ref[...] * p
            - east_ref[...] * to_east(p)
            - west_ref[...] * to_west(p)
            - north_ref[...] * to_north(p)
            - south_ref[...] * to_south(p)
        )
        alpha = product / total(p * image)
        answer = answer + alpha * p_ref[:height, :width]
        r_ref[...] = r_ref[...] - alpha * image
        return answer

    def step(_, carry):
        product, answer = carry
        answer = advance(product, answer)
        search = r_ref[...] * inverse_ref[...]
        new = total(r_ref[...] * search)
        p_ref[...] = search + (new / product) * p_ref[...]
        return new, answer

    product, answer = lax.fori_loop(0, ITERS - 1, step, (product, jnp.zeros((height, width), jnp.float32)))
    height_ref[...] = advance(product, answer)
    residual_ref[...] = r_ref[:height, :width]


def shifted(x, axis, distance):
    count = lax.axis_size(axis)
    return lax.ppermute(x, axis, [((i + distance) % count, i) for i in range(count)])


def per_device(surface_forcing, sea_mask, level_count, state):
    fields, levels, height, width = state.shape
    lats, lons = lax.axis_size("lat"), lax.axis_size("lon")
    block = pick_block(levels)
    f32 = jnp.float32
    pairs = fields // 2
    rows = height + 8
    whole = lambda shape: pl.BlockSpec(shape, lambda i: (0,) * len(shape))
    small = (height + 2, 2, width)
    edge_rows = pl.BlockSpec((fields, block, 2, width), lambda i: (0, i, 0, 0))
    row_shape = jax.ShapeDtypeStruct((fields, levels, 2, width), f32)
    up_rows, down_rows, north_msg, south_msg, pair, cols = pl.pallas_call(
        functools.partial(pack_kernel, levels=levels),
        grid=(levels // block,),
        in_specs=[whole((height, width))] * 3 + [pl.BlockSpec((fields, block, height, width), lambda i: (0, i, 0, 0))],
        out_specs=[edge_rows, edge_rows, whole(small), whole(small), whole((height, 2, width)), whole((4, pairs, height, width))],
        out_shape=[
            row_shape,
            row_shape,
            jax.ShapeDtypeStruct(small, f32),
            jax.ShapeDtypeStruct(small, f32),
            jax.ShapeDtypeStruct((height, 2, width), f32),
            jax.ShapeDtypeStruct((4, pairs, height, width), f32),
        ],
        name="pack",
    )(surface_forcing, sea_mask, level_count, state)

    place = lax.axis_index("lat").astype(jnp.int32)[None]
    from_lat = [
        shifted(south_msg if b == 1 else north_msg if b == lats - 1 else pair, "lat", b) for b in range(1, lats)
    ]
    above = shifted(down_rows, "lat", 1)
    below = shifted(up_rows, "lat", lats - 1)
    smem = pl.BlockSpec(memory_space=pltpu.SMEM)
    vmem = pl.BlockSpec(memory_space=pltpu.VMEM)
    strip = 2 * pairs * rows
    cells = lats * 2 * height
    wide, west_msg, east_msg, grid = pl.pallas_call(
        functools.partial(middle_kernel, levels=levels, fields=fields, lats=lats),
        in_specs=[smem] + [vmem] * (2 + lats - 1),
        out_specs=[vmem] * 4,
        out_shape=[
            jax.ShapeDtypeStruct((rows, width), f32),
            jax.ShapeDtypeStruct((strip + cells, width), f32),
            jax.ShapeDtypeStruct((strip + cells, width), f32),
            jax.ShapeDtypeStruct((cells, width), f32),
        ],
        scratch_shapes=[pltpu.VMEM((rows, width), f32)],
        name="middle",
    )(place, cols, pair, *from_lat)

    order = [1, lons - 1] + list(range(2, lons - 1))
    got = {d: shifted(west_msg if d == 1 else east_msg if d == lons - 1 else grid, "lon", d) for d in order}
    tendency = pl.pallas_call(
        functools.partial(tendency_kernel, levels=levels),
        grid=(levels // block,),
        in_specs=[
            pl.BlockSpec((fields, block, height, width), lambda i: (0, i, 0, 0)),
            edge_rows,
            edge_rows,
            whole((rows, width)),
        ]
        + [whole((strip, width))] * 4,
        out_specs=pl.BlockSpec((fields, block, height, width), lambda i: (0, i, 0, 0)),
        out_shape=jax.ShapeDtypeStruct(state.shape, f32),
        scratch_shapes=[pltpu.VMEM((4, rows, width), f32), pltpu.VMEM((2, pairs, rows, width), f32), pltpu.VMEM((fields, block, 8, width), f32)],
        cost_estimate=pl.CostEstimate(flops=100 * state.size, bytes_accessed=9 * state.size, transcendentals=0),
        name="tendency",
    )(state, below, above, wide, west_msg, east_msg, got[lons - 1], got[1])

    field = pltpu.VMEM((lats * height, lons * width), f32)
    surface, residual = pl.pallas_call(
        functools.partial(solve_kernel, levels=levels, lats=lats, lons=lons, height=height, width=width),
        in_specs=[smem] + [vmem] * lons,
        out_specs=[vmem] * 2,
        out_shape=[jax.ShapeDtypeStruct((height, width), f32)] * 2,
        scratch_shapes=[field] * 8,
        name="solve",
    )(place, grid, *[got[d] for d in range(1, lons)])
    return surface, residual, tendency


def solution(mesh):
    return jax.shard_map(
        per_device,
        mesh=mesh,
        in_specs=(P("lat", "lon"), P("lat", "lon"), P("lat", "lon"), P(None, None, "lat", "lon")),
        out_specs=(P("lat", "lon"), P("lat", "lon"), P(None, None, "lat", "lon")),
        check_vma=False,
    )
```

```python
import functools

import jax
import jax.numpy as jnp
from jax import lax
from jax.experimental import pallas as pl
from jax.experimental.pallas import tpu as pltpu
from jax.sharding import PartitionSpec as P

ITERS = 4
damping = 0.05
viscosity = 0.02
LEVEL_BLOCK = 8
HALF = 64


def lane_iota(shape):
    return lax.broadcasted_iota(jnp.int32, shape, 1)


def pick_block(levels):
    return LEVEL_BLOCK if levels % LEVEL_BLOCK == 0 else 1


def first_kernel(force_ref, sea_ref, count_ref, low_ref, high_ref, north_ref, south_ref, pair_ref):
    fields, levels, band, width = low_ref.shape
    height = force_ref.shape[0]
    sea = sea_ref[...].astype(jnp.float32)
    wet = sea * count_ref[...].astype(jnp.float32)
    forcing = sea * force_ref[...]
    half = height // 2
    for n in range(half):
        rows = slice(2 * n, 2 * n + 2)
        for ref in (north_ref, south_ref, pair_ref):
            ref[n] = forcing[rows]
            ref[half + n] = wet[rows]
    lane = lane_iota((band, width))
    for state_ref, out_ref, row in ((high_ref, north_ref, band - 1), (low_ref, south_ref, 0)):
        held = [[jnp.zeros((band, width), jnp.float32) for _ in range(fields // 2)] for _ in range(2)]
        for f in range(fields):
            for k in range(levels):
                x = state_ref[f, k]
                spot = (f % 2) * HALF + k
                for slot, edge in enumerate((0, width - 1)):
                    moved = pltpu.roll(x, (spot - edge) % width, 1)
                    held[slot][f // 2] = jnp.where(lane == spot, moved, held[slot][f // 2])
        for slot in range(2):
            for p in range(fields // 2):
                out_ref[height + slot, p : p + 1] = held[slot][p][row : row + 1]


def pack_kernel(state_ref, up_ref, down_ref, cols_ref):
    step = pl.program_id(0)
    fields, block, height, width = state_ref.shape

    @pl.when(step == 0)
    def _():
        cols_ref[...] = jnp.zeros(cols_ref.shape, jnp.float32)

    lane = lane_iota((height, width))
    edges = (0, 1, width - 2, width - 1)
    held = [[cols_ref[c, p] for p in range(fields // 2)] for c in range(4)]
    for kk in range(block):
        level = step * block + kk
        for f in range(fields):
            x = state_ref[f, kk]
            up_ref[f, kk] = x[height - 2 :]
            down_ref[f, kk] = x[:2]
            spot = (f % 2) * HALF + level
            mine = lane == spot
            for c, edge in enumerate(edges):
                moved = pltpu.roll(x, lax.rem(spot + (width - edge), width), 1)
                held[c][f // 2] = jnp.where(mine, moved, held[c][f // 2])
    for c in range(4):
        for p in range(fields // 2):
            cols_ref[c, p] = held[c][p]


def middle_kernel(*refs, levels, fields, lats):
    place_ref, cols_ref, own_ref = refs[:3]
    others = refs[3 : 3 + lats - 1]
    wide_ref, west_ref, east_ref, grid_ref, tall = refs[3 + lats - 1 :]
    height, width = cols_ref.shape[2:]
    half = height // 2
    north, south = others[0], others[lats - 2]
    for b in range(lats):
        source = own_ref if b == 0 else others[b - 1]
        for n in range(height):
            grid_ref[b * 2 * height + 2 * n : b * 2 * height + 2 * n + 2] = source[n]
    lat = place_ref[0]
    wide_ref[:height] = grid_ref[height : 2 * height]
    wide_ref[height:] = jnp.zeros((8, width), jnp.float32)

    @pl.when(lat < lats - 1)
    def _():
        wide_ref[height : height + 2] = north[half]

    @pl.when(lat > 0)
    def _():
        wide_ref[height + 6 : height + 8] = south[height - 1]

    tall_rows = height + 8
    wide = wide_ref[...]
    lane_tall = lane_iota((tall_rows, width))
    for out_ref, c_near, c_far, edge_near, edge_far, slot in (
        (west_ref, 0, 1, 0, 1, 0),
        (east_ref, 3, 2, width - 1, width - 2, 1),
    ):
        for p in range(fields // 2):
            tall[:height] = cols_ref[c_near, p]
            tall[height:] = jnp.zeros((8, width), jnp.float32)
            tall[height : height + 1] = north[height + slot, p : p + 1]
            tall[height + 7 :] = south[height + slot, p : p + 1]
            value = tall[...]
            tall[:height] = cols_ref[c_far, p]
            tall[height:] = jnp.zeros((8, width), jnp.float32)
            value_far = tall[...]
            if p == 0:
                value = jnp.where(lane_tall == levels, pltpu.roll(wide, (levels - edge_near) % width, 1), value)
                value_far = jnp.where(lane_tall == levels, pltpu.roll(wide, (levels - edge_far) % width, 1), value_far)
            out_ref[p * tall_rows : (p + 1) * tall_rows] = value
            q = fields // 2 + p
            out_ref[q * tall_rows : (q + 1) * tall_rows] = value_far
        out_ref[2 * (fields // 2) * tall_rows :] = grid_ref[...]


def tendency_kernel(
    state_ref, below_ref, above_ref, wide_ref, own_w_ref, own_e_ref, got_w_ref, got_e_ref, out_ref, faces, edge_lap, halo, *, levels
):
    step = pl.program_id(0)
    fields, block, height, width = state_ref.shape
    rows = height + 8
    pairs = fields // 2
    lane = lane_iota((rows, width))
    last, first = lane == width - 1, lane == 0

    def part(ref, far, p):
        q = (pairs if far else 0) + p
        return ref[q * rows : (q + 1) * rows]

    def up(x):
        return pltpu.roll(x, rows - 1, 0)

    def down(x):
        return pltpu.roll(x, 1, 0)

    @pl.when(step == 0)
    def _():
        halo[...] = jnp.zeros(halo.shape, jnp.float32)
        wide = wide_ref[...]
        east = jnp.where(last, pltpu.roll(part(got_e_ref, False, 0), width - 1 - levels, 1), pltpu.roll(wide, width - 1, 1))
        west = jnp.where(first, pltpu.roll(part(got_w_ref, False, 0), width - levels, 1), pltpu.roll(wide, 1, 1))
        for n, other in enumerate((east, west, up(wide), down(wide))):
            faces[n] = jnp.minimum(wide, other)
        depth_at = lax.rem(lane, HALF).astype(jnp.float32)
        for side, (got, own, sign) in enumerate(((got_w_ref, own_w_ref, 1.0), (got_e_ref, own_e_ref, -1.0))):
            wet_near, wet_far, wet_own = (
                jnp.broadcast_to(part(ref, far, 0)[:, levels : levels + 1], (rows, width))
                for ref, far in ((got, False), (got, True), (own, False))
            )
            masks = [depth_at < jnp.minimum(wet_near, other) for other in (wet_own, wet_far, up(wet_near), down(wet_near))]
            for p in range(pairs):
                here, beyond, inner = part(got, False, p), part(got, True, p), part(own, False, p)
                total = jnp.zeros((rows, width), jnp.float32)
                for mask, other in zip(masks, (inner, beyond, up(here), down(here))):
                    total = total + jnp.where(mask, other - here, 0.0)
                edge_lap[side, p] = total

    wide = wide_ref[...]
    low = slice(0, height)
    for kk in range(block):
        for f in range(fields):
            halo[f, kk, 0:2] = above_ref[f, kk]
            halo[f, kk, 6:8] = below_ref[f, kk]
    for kk in range(block):
        level = step * block + kk
        depth = level.astype(jnp.float32)
        on_e, on_w, on_n, on_s = (depth < faces[n] for n in range(4))
        here_on = depth < wide[low]
        around = []
        for f in range(fields):
            x = jnp.concatenate([state_ref[f, kk], halo[f, kk]], axis=0)
            spot = (f % 2) * HALF + level
            p = f // 2
            east = jnp.where(last, pltpu.roll(part(got_e_ref, False, p), width - 1 - spot, 1), pltpu.roll(x, width - 1, 1))
            west = jnp.where(first, pltpu.roll(part(got_w_ref, False, p), lax.rem(width - spot, width), 1), pltpu.roll(x, 1, 1))
            around.append((x, east, west, up(x), down(x)))
        u, v = around[2], around[3]
        mask_low = [m[low] for m in (on_e, on_w, on_n, on_s)]
        speed = [
            jnp.where(mask_low[0], 0.25 * (u[0][low] + u[1][low]), 0.0),
            jnp.where(mask_low[1], 0.25 * (u[0][low] + u[2][low]), 0.0),
            jnp.where(mask_low[2], 0.25 * (v[0][low] + v[3][low]), 0.0),
            jnp.where(mask_low[3], 0.25 * (v[0][low] + v[4][low]), 0.0),
        ]
        for f in range(fields):
            x, east, west, north, south = around[f]
            spot = (f % 2) * HALF + level
            p = f // 2
            lap = (
                jnp.where(on_e, east - x, 0.0)
                - jnp.where(on_w, x - west, 0.0)
                + jnp.where(on_n, north - x, 0.0)
                - jnp.where(on_s, x - south, 0.0)
            )
            inner = lap[low]
            lap_e = jnp.where(last[low], pltpu.roll(edge_lap[1, p][low], width - 1 - spot, 1), pltpu.roll(inner, width - 1, 1))
            lap_w = jnp.where(first[low], pltpu.roll(edge_lap[0, p][low], lax.rem(width - spot, width), 1), pltpu.roll(inner, 1, 1))
            lap_n, lap_s = up(lap)[low], down(lap)[low]
            second = (
                jnp.where(mask_low[0], lap_e - inner, 0.0)
                - jnp.where(mask_low[1], inner - lap_w, 0.0)
                + jnp.where(mask_low[2], lap_n - inner, 0.0)
                - jnp.where(mask_low[3], inner - lap_s, 0.0)
            )
            q = x[low]
            flux = (
                speed[0] * (q + east[low])
                - speed[1] * (q + west[low])
                + speed[2] * (q + north[low])
                - speed[3] * (q + south[low])
            )
            out_ref[f, kk] = jnp.where(here_on, -flux - viscosity * second, 0.0)


def solve_kernel(*refs, levels, lats, lons, height, width):
    place_ref = refs[0]
    sources = refs[1 : 1 + lons]
    height_ref, residual_ref = refs[1 + lons : 3 + lons]
    depth_ref, east_ref, west_ref, north_ref, south_ref, diag_ref, r_ref, p_ref = refs[3 + lons :]
    tall, broad = lats * height, lons * width
    for d, source in enumerate(sources):
        start = source.shape[0] - lats * 2 * height
        for b in range(lats):
            at = start + b * 2 * height
            block = (slice(b * height, (b + 1) * height), slice(d * width, (d + 1) * width))
            r_ref[block] = source[at : at + height]
            depth_ref[block] = source[at + height : at + 2 * height] / levels

    def to_east(x):
        return pltpu.roll(x, broad - 1, 1)

    def to_west(x):
        return pltpu.roll(x, 1, 1)

    def to_north(x):
        return pltpu.roll(x, tall - 1, 0)

    def to_south(x):
        return pltpu.roll(x, 1, 0)

    depth = depth_ref[...]
    row = lax.rem(lax.broadcasted_iota(jnp.int32, (tall, broad), 0) + place_ref[0] * height, tall)
    east_ref[...] = jnp.minimum(depth, to_east(depth))
    west_ref[...] = jnp.minimum(depth, to_west(depth))
    north_ref[...] = jnp.where(row == tall - 1, 0.0, jnp.minimum(depth, to_north(depth)))
    south_ref[...] = jnp.where(row == 0, 0.0, jnp.minimum(depth, to_south(depth)))
    diag_ref[...] = damping + east_ref[...] + west_ref[...] + north_ref[...] + south_ref[...]
    depth_ref[...] = 1.0 / diag_ref[...]
    inverse_ref = depth_ref
    search = r_ref[...] * inverse_ref[...]
    p_ref[...] = search

    def total(x):
        return jnp.sum(jnp.sum(x, axis=0, keepdims=True), axis=1, keepdims=True)

    product = total(r_ref[...] * search)

    def advance(product, answer):
        p = p_ref[...]
        image = (
            diag_ref[...] * p
            - east_ref[...] * to_east(p)
            - west_ref[...] * to_west(p)
            - north_ref[...] * to_north(p)
            - south_ref[...] * to_south(p)
        )
        alpha = product / total(p * image)
        answer = answer + alpha * p_ref[:height, :width]
        r_ref[...] = r_ref[...] - alpha * image
        return answer

    def step(_, carry):
        product, answer = carry
        answer = advance(product, answer)
        search = r_ref[...] * inverse_ref[...]
        new = total(r_ref[...] * search)
        p_ref[...] = search + (new / product) * p_ref[...]
        return new, answer

    product, answer = lax.fori_loop(0, ITERS - 1, step, (product, jnp.zeros((height, width), jnp.float32)))
    height_ref[...] = advance(product, answer)
    residual_ref[...] = r_ref[:height, :width]


def shifted(x, axis, distance):
    count = lax.axis_size(axis)
    return lax.ppermute(x, axis, [((i + distance) % count, i) for i in range(count)])


def per_device(surface_forcing, sea_mask, level_count, state):
    fields, levels, height, width = state.shape
    lats, lons = lax.axis_size("lat"), lax.axis_size("lon")
    block = pick_block(levels)
    f32 = jnp.float32
    pairs = fields // 2
    rows = height + 8
    whole = lambda shape: pl.BlockSpec(shape, lambda i: (0,) * len(shape))
    small = (height + 2, 2, width)
    edge_rows = pl.BlockSpec((fields, block, 2, width), lambda i: (0, i, 0, 0))
    row_shape = jax.ShapeDtypeStruct((fields, levels, 2, width), f32)
    band = 8
    cells_block = whole((height, width))
    north_msg, south_msg, pair = pl.pallas_call(
        first_kernel,
        grid=(1,),
        in_specs=[cells_block] * 3
        + [
            pl.BlockSpec((fields, levels, band, width), lambda i: (0, 0, 0, 0)),
            pl.BlockSpec((fields, levels, band, width), lambda i: (0, 0, height // band - 1, 0)),
        ],
        out_specs=[whole(small), whole(small), whole((height, 2, width))],
        out_shape=[
            jax.ShapeDtypeStruct(small, f32),
            jax.ShapeDtypeStruct(small, f32),
            jax.ShapeDtypeStruct((height, 2, width), f32),
        ],
        name="first",
    )(surface_forcing, sea_mask, level_count, state, state)
    up_rows, down_rows, cols = pl.pallas_call(
        pack_kernel,
        grid=(levels // block,),
        in_specs=[pl.BlockSpec((fields, block, height, width), lambda i: (0, i, 0, 0))],
        out_specs=[edge_rows, edge_rows, whole((4, pairs, height, width))],
        out_shape=[row_shape, row_shape, jax.ShapeDtypeStruct((4, pairs, height, width), f32)],
        cost_estimate=pl.CostEstimate(flops=100 * state.size, bytes_accessed=5 * state.size, transcendentals=0),
        name="pack",
    )(state)

    place = lax.axis_index("lat").astype(jnp.int32)[None]
    from_lat = [
        shifted(south_msg if b == 1 else north_msg if b == lats - 1 else pair, "lat", b) for b in range(1, lats)
    ]
    above = shifted(down_rows, "lat", 1)
    below = shifted(up_rows, "lat", lats - 1)
    smem = pl.BlockSpec(memory_space=pltpu.SMEM)
    vmem = pl.BlockSpec(memory_space=pltpu.VMEM)
    strip = 2 * pairs * rows
    cells = lats * 2 * height
    wide, west_msg, east_msg, grid = pl.pallas_call(
        functools.partial(middle_kernel, levels=levels, fields=fields, lats=lats),
        in_specs=[smem] + [vmem] * (2 + lats - 1),
        out_specs=[vmem] * 4,
        out_shape=[
            jax.ShapeDtypeStruct((rows, width), f32),
            jax.ShapeDtypeStruct((strip + cells, width), f32),
            jax.ShapeDtypeStruct((strip + cells, width), f32),
            jax.ShapeDtypeStruct((cells, width), f32),
        ],
        scratch_shapes=[pltpu.VMEM((rows, width), f32)],
        name="middle",
    )(place, cols, pair, *from_lat)

    order = [1, lons - 1] + list(range(2, lons - 1))
    got = {d: shifted(west_msg if d == 1 else east_msg if d == lons - 1 else grid, "lon", d) for d in order}
    tendency = pl.pallas_call(
        functools.partial(tendency_kernel, levels=levels),
        grid=(levels // block,),
        in_specs=[
            pl.BlockSpec((fields, block, height, width), lambda i: (0, i, 0, 0)),
            edge_rows,
            edge_rows,
            whole((rows, width)),
        ]
        + [whole((strip, width))] * 4,
        out_specs=pl.BlockSpec((fields, block, height, width), lambda i: (0, i, 0, 0)),
        out_shape=jax.ShapeDtypeStruct(state.shape, f32),
        scratch_shapes=[pltpu.VMEM((4, rows, width), f32), pltpu.VMEM((2, pairs, rows, width), f32), pltpu.VMEM((fields, block, 8, width), f32)],
        cost_estimate=pl.CostEstimate(flops=100 * state.size, bytes_accessed=9 * state.size, transcendentals=0),
        name="tendency",
    )(state, below, above, wide, west_msg, east_msg, got[lons - 1], got[1])

    field = pltpu.VMEM((lats * height, lons * width), f32)
    surface, residual = pl.pallas_call(
        functools.partial(solve_kernel, levels=levels, lats=lats, lons=lons, height=height, width=width),
        in_specs=[smem] + [vmem] * lons,
        out_specs=[vmem] * 2,
        out_shape=[jax.ShapeDtypeStruct((height, width), f32)] * 2,
        scratch_shapes=[field] * 8,
        name="solve",
    )(place, grid, *[got[d] for d in range(1, lons)])
    return surface, residual, tendency


def solution(mesh):
    return jax.shard_map(
        per_device,
        mesh=mesh,
        in_specs=(P("lat", "lon"), P("lat", "lon"), P("lat", "lon"), P(None, None, "lat", "lon")),
        out_specs=(P("lat", "lon"), P("lat", "lon"), P(None, None, "lat", "lon")),
        check_vma=False,
    )
```

```python
import functools

import jax
import jax.numpy as jnp
from jax import lax
from jax.experimental import pallas as pl
from jax.experimental.pallas import tpu as pltpu
from jax.sharding import PartitionSpec as P

ITERS = 4
damping = 0.05
viscosity = 0.02
LEVEL_BLOCK = 4
HALF = 64


def lane_iota(shape):
    return lax.broadcasted_iota(jnp.int32, shape, 1)


def pick_block(levels):
    return LEVEL_BLOCK if levels % LEVEL_BLOCK == 0 else 1


def first_kernel(force_ref, sea_ref, count_ref, low_ref, high_ref, north_ref, south_ref, pair_ref):
    fields, levels, band, width = low_ref.shape
    height = force_ref.shape[0]
    sea = sea_ref[...].astype(jnp.float32)
    wet = sea * count_ref[...].astype(jnp.float32)
    forcing = sea * force_ref[...]
    half = height // 2
    for n in range(half):
        rows = slice(2 * n, 2 * n + 2)
        for ref in (north_ref, south_ref, pair_ref):
            ref[n] = forcing[rows]
            ref[half + n] = wet[rows]
    lane = lane_iota((band, width))
    for state_ref, out_ref, row in ((high_ref, north_ref, band - 1), (low_ref, south_ref, 0)):
        held = [[jnp.zeros((band, width), jnp.float32) for _ in range(fields // 2)] for _ in range(2)]
        for f in range(fields):
            for k in range(levels):
                x = state_ref[f, k]
                spot = (f % 2) * HALF + k
                for slot, edge in enumerate((0, width - 1)):
                    moved = pltpu.roll(x, (spot - edge) % width, 1)
                    held[slot][f // 2] = jnp.where(lane == spot, moved, held[slot][f // 2])
        for slot in range(2):
            for p in range(fields // 2):
                out_ref[height + slot, p : p + 1] = held[slot][p][row : row + 1]


def pack_kernel(state_ref, up_ref, down_ref, cols_ref):
    step = pl.program_id(0)
    fields, block, height, width = state_ref.shape

    @pl.when(step == 0)
    def _():
        cols_ref[...] = jnp.zeros(cols_ref.shape, jnp.float32)

    lane = lane_iota((height, width))
    edges = (0, 1, width - 2, width - 1)
    held = [[cols_ref[c, p] for p in range(fields // 2)] for c in range(4)]
    for kk in range(block):
        level = step * block + kk
        for f in range(fields):
            x = state_ref[f, kk]
            up_ref[f, kk] = x[height - 2 :]
            down_ref[f, kk] = x[:2]
            spot = (f % 2) * HALF + level
            mine = lane == spot
            for c, edge in enumerate(edges):
                moved = pltpu.roll(x, lax.rem(spot + (width - edge), width), 1)
                held[c][f // 2] = jnp.where(mine, moved, held[c][f // 2])
    for c in range(4):
        for p in range(fields // 2):
            cols_ref[c, p] = held[c][p]


def middle_kernel(*refs, levels, fields, lats):
    place_ref, cols_ref, own_ref = refs[:3]
    others = refs[3 : 3 + lats - 1]
    wide_ref, west_ref, east_ref, grid_ref, tall = refs[3 + lats - 1 :]
    height, width = cols_ref.shape[2:]
    half = height // 2
    north, south = others[0], others[lats - 2]
    for b in range(lats):
        source = own_ref if b == 0 else others[b - 1]
        for n in range(height):
            grid_ref[b * 2 * height + 2 * n : b * 2 * height + 2 * n + 2] = source[n]
    lat = place_ref[0]
    wide_ref[:height] = grid_ref[height : 2 * height]
    wide_ref[height:] = jnp.zeros((8, width), jnp.float32)

    @pl.when(lat < lats - 1)
    def _():
        wide_ref[height : height + 2] = north[half]

    @pl.when(lat > 0)
    def _():
        wide_ref[height + 6 : height + 8] = south[height - 1]

    tall_rows = height + 8
    wide = wide_ref[...]
    lane_tall = lane_iota((tall_rows, width))
    for out_ref, c_near, c_far, edge_near, edge_far, slot in (
        (west_ref, 0, 1, 0, 1, 0),
        (east_ref, 3, 2, width - 1, width - 2, 1),
    ):
        for p in range(fields // 2):
            tall[:height] = cols_ref[c_near, p]
            tall[height:] = jnp.zeros((8, width), jnp.float32)
            tall[height : height + 1] = north[height + slot, p : p + 1]
            tall[height + 7 :] = south[height + slot, p : p + 1]
            value = tall[...]
            tall[:height] = cols_ref[c_far, p]
            tall[height:] = jnp.zeros((8, width), jnp.float32)
            value_far = tall[...]
            if p == 0:
                value = jnp.where(lane_tall == levels, pltpu.roll(wide, (levels - edge_near) % width, 1), value)
                value_far = jnp.where(lane_tall == levels, pltpu.roll(wide, (levels - edge_far) % width, 1), value_far)
            out_ref[p * tall_rows : (p + 1) * tall_rows] = value
            q = fields // 2 + p
            out_ref[q * tall_rows : (q + 1) * tall_rows] = value_far
        out_ref[2 * (fields // 2) * tall_rows :] = grid_ref[...]


def tendency_kernel(
    state_ref, below_ref, above_ref, wide_ref, own_w_ref, own_e_ref, got_w_ref, got_e_ref, out_ref, faces, edge_lap, halo, *, levels
):
    step = pl.program_id(0)
    fields, block, height, width = state_ref.shape
    rows = height + 8
    pairs = fields // 2
    lane = lane_iota((rows, width))
    last, first = lane == width - 1, lane == 0

    def part(ref, far, p):
        q = (pairs if far else 0) + p
        return ref[q * rows : (q + 1) * rows]

    def up(x):
        return pltpu.roll(x, rows - 1, 0)

    def down(x):
        return pltpu.roll(x, 1, 0)

    @pl.when(step == 0)
    def _():
        halo[...] = jnp.zeros(halo.shape, jnp.float32)
        wide = wide_ref[...]
        east = jnp.where(last, pltpu.roll(part(got_e_ref, False, 0), width - 1 - levels, 1), pltpu.roll(wide, width - 1, 1))
        west = jnp.where(first, pltpu.roll(part(got_w_ref, False, 0), width - levels, 1), pltpu.roll(wide, 1, 1))
        for n, other in enumerate((east, west, up(wide), down(wide))):
            faces[n] = jnp.minimum(wide, other)
        depth_at = lax.rem(lane, HALF).astype(jnp.float32)
        for side, (got, own, sign) in enumerate(((got_w_ref, own_w_ref, 1.0), (got_e_ref, own_e_ref, -1.0))):
            wet_near, wet_far, wet_own = (
                jnp.broadcast_to(part(ref, far, 0)[:, levels : levels + 1], (rows, width))
                for ref, far in ((got, False), (got, True), (own, False))
            )
            masks = [depth_at < jnp.minimum(wet_near, other) for other in (wet_own, wet_far, up(wet_near), down(wet_near))]
            for p in range(pairs):
                here, beyond, inner = part(got, False, p), part(got, True, p), part(own, False, p)
                total = jnp.zeros((rows, width), jnp.float32)
                for mask, other in zip(masks, (inner, beyond, up(here), down(here))):
                    total = total + jnp.where(mask, other - here, 0.0)
                edge_lap[side, p] = total

    wide = wide_ref[...]
    low = slice(0, height)
    for kk in range(block):
        for f in range(fields):
            halo[f, kk, 0:2] = above_ref[f, kk]
            halo[f, kk, 6:8] = below_ref[f, kk]
    for kk in range(block):
        level = step * block + kk
        depth = level.astype(jnp.float32)
        on_e, on_w, on_n, on_s = (depth < faces[n] for n in range(4))
        here_on = depth < wide[low]
        around = []
        for f in range(fields):
            x = jnp.concatenate([state_ref[f, kk], halo[f, kk]], axis=0)
            spot = (f % 2) * HALF + level
            p = f // 2
            east = jnp.where(last, pltpu.roll(part(got_e_ref, False, p), width - 1 - spot, 1), pltpu.roll(x, width - 1, 1))
            west = jnp.where(first, pltpu.roll(part(got_w_ref, False, p), lax.rem(width - spot, width), 1), pltpu.roll(x, 1, 1))
            around.append((x, east, west, up(x), down(x)))
        u, v = around[2], around[3]
        mask_low = [m[low] for m in (on_e, on_w, on_n, on_s)]
        speed = [
            jnp.where(mask_low[0], 0.25 * (u[0][low] + u[1][low]), 0.0),
            jnp.where(mask_low[1], 0.25 * (u[0][low] + u[2][low]), 0.0),
            jnp.where(mask_low[2], 0.25 * (v[0][low] + v[3][low]), 0.0),
            jnp.where(mask_low[3], 0.25 * (v[0][low] + v[4][low]), 0.0),
        ]
        for f in range(fields):
            x, east, west, north, south = around[f]
            spot = (f % 2) * HALF + level
            p = f // 2
            lap = (
                jnp.where(on_e, east - x, 0.0)
                - jnp.where(on_w, x - west, 0.0)
                + jnp.where(on_n, north - x, 0.0)
                - jnp.where(on_s, x - south, 0.0)
            )
            inner = lap[low]
            lap_e = jnp.where(last[low], pltpu.roll(edge_lap[1, p][low], width - 1 - spot, 1), pltpu.roll(inner, width - 1, 1))
            lap_w = jnp.where(first[low], pltpu.roll(edge_lap[0, p][low], lax.rem(width - spot, width), 1), pltpu.roll(inner, 1, 1))
            lap_n, lap_s = up(lap)[low], down(lap)[low]
            second = (
                jnp.where(mask_low[0], lap_e - inner, 0.0)
                - jnp.where(mask_low[1], inner - lap_w, 0.0)
                + jnp.where(mask_low[2], lap_n - inner, 0.0)
                - jnp.where(mask_low[3], inner - lap_s, 0.0)
            )
            q = x[low]
            flux = (
                speed[0] * (q + east[low])
                - speed[1] * (q + west[low])
                + speed[2] * (q + north[low])
                - speed[3] * (q + south[low])
            )
            out_ref[f, kk] = jnp.where(here_on, -flux - viscosity * second, 0.0)


def solve_kernel(*refs, levels, lats, lons, height, width):
    place_ref = refs[0]
    sources = refs[1 : 1 + lons]
    height_ref, residual_ref = refs[1 + lons : 3 + lons]
    depth_ref, east_ref, west_ref, north_ref, south_ref, diag_ref, r_ref, p_ref = refs[3 + lons :]
    tall, broad = lats * height, lons * width
    for d, source in enumerate(sources):
        start = source.shape[0] - lats * 2 * height
        for b in range(lats):
            at = start + b * 2 * height
            block = (slice(b * height, (b + 1) * height), slice(d * width, (d + 1) * width))
            r_ref[block] = source[at : at + height]
            depth_ref[block] = source[at + height : at + 2 * height] / levels

    def to_east(x):
        return pltpu.roll(x, broad - 1, 1)

    def to_west(x):
        return pltpu.roll(x, 1, 1)

    def to_north(x):
        return pltpu.roll(x, tall - 1, 0)

    def to_south(x):
        return pltpu.roll(x, 1, 0)

    depth = depth_ref[...]
    row = lax.rem(lax.broadcasted_iota(jnp.int32, (tall, broad), 0) + place_ref[0] * height, tall)
    east_ref[...] = jnp.minimum(depth, to_east(depth))
    west_ref[...] = jnp.minimum(depth, to_west(depth))
    north_ref[...] = jnp.where(row == tall - 1, 0.0, jnp.minimum(depth, to_north(depth)))
    south_ref[...] = jnp.where(row == 0, 0.0, jnp.minimum(depth, to_south(depth)))
    diag_ref[...] = damping + east_ref[...] + west_ref[...] + north_ref[...] + south_ref[...]
    depth_ref[...] = 1.0 / diag_ref[...]
    inverse_ref = depth_ref
    search = r_ref[...] * inverse_ref[...]
    p_ref[...] = search

    def total(x):
        return jnp.sum(jnp.sum(x, axis=0, keepdims=True), axis=1, keepdims=True)

    product = total(r_ref[...] * search)

    def advance(product, answer):
        p = p_ref[...]
        image = (
            diag_ref[...] * p
            - east_ref[...] * to_east(p)
            - west_ref[...] * to_west(p)
            - north_ref[...] * to_north(p)
            - south_ref[...] * to_south(p)
        )
        alpha = product / total(p * image)
        answer = answer + alpha * p_ref[:height, :width]
        r_ref[...] = r_ref[...] - alpha * image
        return answer

    def step(_, carry):
        product, answer = carry
        answer = advance(product, answer)
        search = r_ref[...] * inverse_ref[...]
        new = total(r_ref[...] * search)
        p_ref[...] = search + (new / product) * p_ref[...]
        return new, answer

    product, answer = lax.fori_loop(0, ITERS - 1, step, (product, jnp.zeros((height, width), jnp.float32)))
    height_ref[...] = advance(product, answer)
    residual_ref[...] = r_ref[:height, :width]


def shifted(x, axis, distance):
    count = lax.axis_size(axis)
    return lax.ppermute(x, axis, [((i + distance) % count, i) for i in range(count)])


def per_device(surface_forcing, sea_mask, level_count, state):
    fields, levels, height, width = state.shape
    lats, lons = lax.axis_size("lat"), lax.axis_size("lon")
    block = pick_block(levels)
    f32 = jnp.float32
    pairs = fields // 2
    rows = height + 8
    whole = lambda shape: pl.BlockSpec(shape, lambda i: (0,) * len(shape))
    small = (height + 2, 2, width)
    edge_rows = pl.BlockSpec((fields, block, 2, width), lambda i: (0, i, 0, 0))
    row_shape = jax.ShapeDtypeStruct((fields, levels, 2, width), f32)
    band = 8
    cells_block = whole((height, width))
    north_msg, south_msg, pair = pl.pallas_call(
        first_kernel,
        grid=(1,),
        in_specs=[cells_block] * 3
        + [
            pl.BlockSpec((fields, levels, band, width), lambda i: (0, 0, 0, 0)),
            pl.BlockSpec((fields, levels, band, width), lambda i: (0, 0, height // band - 1, 0)),
        ],
        out_specs=[whole(small), whole(small), whole((height, 2, width))],
        out_shape=[
            jax.ShapeDtypeStruct(small, f32),
            jax.ShapeDtypeStruct(small, f32),
            jax.ShapeDtypeStruct((height, 2, width), f32),
        ],
        name="first",
    )(surface_forcing, sea_mask, level_count, state, state)
    up_rows, down_rows, cols = pl.pallas_call(
        pack_kernel,
        grid=(levels // block,),
        in_specs=[pl.BlockSpec((fields, block, height, width), lambda i: (0, i, 0, 0))],
        out_specs=[edge_rows, edge_rows, whole((4, pairs, height, width))],
        out_shape=[row_shape, row_shape, jax.ShapeDtypeStruct((4, pairs, height, width), f32)],
        cost_estimate=pl.CostEstimate(flops=100 * state.size, bytes_accessed=5 * state.size, transcendentals=0),
        name="pack",
    )(state)

    place = lax.axis_index("lat").astype(jnp.int32)[None]
    from_lat = [
        shifted(south_msg if b == 1 else north_msg if b == lats - 1 else pair, "lat", b) for b in range(1, lats)
    ]
    above = shifted(down_rows, "lat", 1)
    below = shifted(up_rows, "lat", lats - 1)
    smem = pl.BlockSpec(memory_space=pltpu.SMEM)
    vmem = pl.BlockSpec(memory_space=pltpu.VMEM)
    strip = 2 * pairs * rows
    cells = lats * 2 * height
    wide, west_msg, east_msg, grid = pl.pallas_call(
        functools.partial(middle_kernel, levels=levels, fields=fields, lats=lats),
        in_specs=[smem] + [vmem] * (2 + lats - 1),
        out_specs=[vmem] * 4,
        out_shape=[
            jax.ShapeDtypeStruct((rows, width), f32),
            jax.ShapeDtypeStruct((strip + cells, width), f32),
            jax.ShapeDtypeStruct((strip + cells, width), f32),
            jax.ShapeDtypeStruct((cells, width), f32),
        ],
        scratch_shapes=[pltpu.VMEM((rows, width), f32)],
        name="middle",
    )(place, cols, pair, *from_lat)

    order = [1, lons - 1] + list(range(2, lons - 1))
    got = {d: shifted(west_msg if d == 1 else east_msg if d == lons - 1 else grid, "lon", d) for d in order}
    tendency = pl.pallas_call(
        functools.partial(tendency_kernel, levels=levels),
        grid=(levels // block,),
        in_specs=[
            pl.BlockSpec((fields, block, height, width), lambda i: (0, i, 0, 0)),
            edge_rows,
            edge_rows,
            whole((rows, width)),
        ]
        + [whole((strip, width))] * 4,
        out_specs=pl.BlockSpec((fields, block, height, width), lambda i: (0, i, 0, 0)),
        out_shape=jax.ShapeDtypeStruct(state.shape, f32),
        scratch_shapes=[pltpu.VMEM((4, rows, width), f32), pltpu.VMEM((2, pairs, rows, width), f32), pltpu.VMEM((fields, block, 8, width), f32)],
        cost_estimate=pl.CostEstimate(flops=100 * state.size, bytes_accessed=9 * state.size, transcendentals=0),
        name="tendency",
    )(state, below, above, wide, west_msg, east_msg, got[lons - 1], got[1])

    field = pltpu.VMEM((lats * height, lons * width), f32)
    surface, residual = pl.pallas_call(
        functools.partial(solve_kernel, levels=levels, lats=lats, lons=lons, height=height, width=width),
        in_specs=[smem] + [vmem] * lons,
        out_specs=[vmem] * 2,
        out_shape=[jax.ShapeDtypeStruct((height, width), f32)] * 2,
        scratch_shapes=[field] * 8,
        name="solve",
    )(place, grid, *[got[d] for d in range(1, lons)])
    return surface, residual, tendency


def solution(mesh):
    return jax.shard_map(
        per_device,
        mesh=mesh,
        in_specs=(P("lat", "lon"), P("lat", "lon"), P("lat", "lon"), P(None, None, "lat", "lon")),
        out_specs=(P("lat", "lon"), P("lat", "lon"), P(None, None, "lat", "lon")),
        check_vma=False,
    )
```
